8 devices in a mesh: dp: 1 (over z), tp: 2 (over y), cp: 4 (over x, core).
Axes of the slice: x: 2, y: 2, z: 1, core: 2. Of those that a mesh axis runs over, the one named last changes fastest.
Arguments:
- hidden: bfloat16 [24, 768, 512], P('dp', 'cp')
- tokens: int32 [24, 768], P('dp', 'cp')
- emb_table: bfloat16 [50304, 512], P('tp')
- out_table: bfloat16 [50304, 512], P('tp')
- w_proj: bfloat16 [512, 1024], replicated
- gain_h: float32 [512], replicated
- gain_e: float32 [512], replicated
- gain_f: float32 [512], replicated
Outputs:
- output 1: float32 [1], P('dp')
- output 2: bfloat16 [24, 768, 512], P('dp', 'cp')
- output 3: float32 [512, 1024], P('dp')
- output 4: float32 [50304, 512], P(('dp', 'tp'))
- output 5: float32 [50304, 512], P(('dp', 'tp'))
- output 6: float32 [512], P('dp')
- output 7: float32 [512], P('dp')
- output 8: float32 [512], P('dp')
All inputs are finite; a program needn't handle non-finite values.
Results may differ from the reference program's by a relative error of at most 0.001.
Values sent between devices are 32-bit elements.
A program may use at most 1 GiB of HBM per device.

```python
import math
import jax
import jax.numpy as jnp
from jax import lax

BATCH_ROWS = 24
SEQ_LEN = 768
MODEL_DIM = 512
VOCAB_SIZE = 50304
MTP_WEIGHT = 0.3
NORM_EPS = 1e-6
ROW_BLOCK = math.gcd(BATCH_ROWS * SEQ_LEN, 512)


def rms_norm(values, gain):
    scale = lax.rsqrt(jnp.mean(values * values, axis=-1, keepdims=True) + NORM_EPS)
    return values * scale * gain


def draw_ids(key):
    key_level, key_pick = jax.random.split(key)
    level = jax.random.randint(key_level, (BATCH_ROWS, SEQ_LEN), 0, 8)
    upper = jnp.right_shift(jnp.full((BATCH_ROWS, SEQ_LEN), VOCAB_SIZE, jnp.int32), level)
    tok_ids = jax.random.randint(key_pick, (BATCH_ROWS, SEQ_LEN), 0, upper)
    return tok_ids.at[0, 1].set(VOCAB_SIZE - 1)


def setup_inputs(seed: int = 0, part: int = 0) -> dict:
    root_key = jax.random.key(seed)
    key_list = jax.random.split(root_key, 8)
    part_key = jax.random.fold_in(key_list[0], part)
    key_hidden, key_tokens = jax.random.split(part_key)
    hidden = jax.random.normal(key_hidden, (BATCH_ROWS, SEQ_LEN, MODEL_DIM), jnp.float32)
    emb_table = jax.random.normal(key_list[1], (VOCAB_SIZE, MODEL_DIM), jnp.float32)
    out_table = jax.random.normal(key_list[2], (VOCAB_SIZE, MODEL_DIM), jnp.float32) * (1.5 * MODEL_DIM ** -0.5)
    w_proj = jax.random.normal(key_list[3], (MODEL_DIM, 2 * MODEL_DIM), jnp.float32) * (2 * MODEL_DIM) ** -0.5
    gain_h = 1.0 + 0.25 * jax.random.normal(key_list[4], (MODEL_DIM,), jnp.float32)
    gain_e = 1.0 + 0.25 * jax.random.normal(key_list[5], (MODEL_DIM,), jnp.float32)
    gain_f = 1.0 + 0.25 * jax.random.normal(key_list[6], (MODEL_DIM,), jnp.float32)
    return {
        "hidden": hidden.astype(jnp.bfloat16),
        "tokens": draw_ids(key_tokens),
        "emb_table": emb_table.astype(jnp.bfloat16),
        "out_table": out_table.astype(jnp.bfloat16),
        "w_proj": w_proj.astype(jnp.bfloat16),
        "gain_h": gain_h,
        "gain_e": gain_e,
        "gain_f": gain_f,
    }


def reference(hidden, tokens, emb_table, out_table, w_proj, gain_h, gain_e, gain_f):
    n_blocks = (BATCH_ROWS * SEQ_LEN) // ROW_BLOCK
    positions = jnp.arange(SEQ_LEN)
    pos_weight = jnp.broadcast_to((positions < SEQ_LEN - 2).astype(jnp.float32), (BATCH_ROWS, SEQ_LEN))
    next_ids = jnp.roll(tokens, -1, axis=1)
    label_ids = jnp.roll(tokens, -2, axis=1)
    vocab_range = jnp.arange(VOCAB_SIZE)
    block_inputs = (
        hidden.reshape(n_blocks, ROW_BLOCK, MODEL_DIM),
        next_ids.reshape(n_blocks, ROW_BLOCK),
        label_ids.reshape(n_blocks, ROW_BLOCK),
        pos_weight.reshape(n_blocks, ROW_BLOCK),
    )

    def block_step(carry, block):
        d_out, d_emb, d_proj, d_gain_h, d_gain_e, d_gain_f, loss_sum = carry
        hid_blk, next_blk, label_blk, weight_blk = block
        hid_f32 = hid_blk.astype(jnp.float32)
        emb_f32 = jnp.take(emb_table, next_blk, axis=0).astype(jnp.float32)
        norm_h, vjp_h = jax.vjp(rms_norm, hid_f32, gain_h)
        norm_e, vjp_e = jax.vjp(rms_norm, emb_f32, gain_e)
        joined = jnp.concatenate([norm_h.astype(jnp.bfloat16), norm_e.astype(jnp.bfloat16)], axis=1)
        mixed = jnp.dot(joined, w_proj.T, preferred_element_type=jnp.float32)
        normed, vjp_f = jax.vjp(rms_norm, mixed, gain_f)
        features = normed.astype(jnp.bfloat16)
        logits = jnp.dot(features, out_table.T, preferred_element_type=jnp.float32)
        row_max = jnp.max(logits, axis=1, keepdims=True)
        log_norm = row_max[:, 0] + jnp.log(jnp.sum(jnp.exp(logits - row_max), axis=1))
        is_label = vocab_range[None, :] == label_blk[:, None]
        label_logit = jnp.sum(jnp.where(is_label, logits, 0.0), axis=1)
        loss_sum = loss_sum + jnp.sum(weight_blk * (log_norm - label_logit))
        soft_prob = jnp.exp(logits - log_norm[:, None])
        grad_logits = (MTP_WEIGHT * weight_blk[:, None] * (soft_prob - is_label.astype(jnp.float32))).astype(jnp.bfloat16)
        d_out = d_out + jnp.dot(grad_logits.T, features, preferred_element_type=jnp.float32)
        d_feats = jnp.dot(grad_logits, out_table, preferred_element_type=jnp.float32)
        d_mixed, grad_gf = vjp_f(d_feats)
        d_mixed_b = d_mixed.astype(jnp.bfloat16)
        d_proj = d_proj + jnp.dot(d_mixed_b.T, joined, preferred_element_type=jnp.float32)
        d_joined = jnp.dot(d_mixed_b, w_proj, preferred_element_type=jnp.float32)
        d_hid, grad_gh = vjp_h(d_joined[:, :MODEL_DIM])
        d_embrow, grad_ge = vjp_e(d_joined[:, MODEL_DIM:])
        d_emb = d_emb.at[next_blk].add(d_embrow)
        new_carry = (d_out, d_emb, d_proj, d_gain_h + grad_gh, d_gain_e + grad_ge, d_gain_f + grad_gf, loss_sum)
        return new_carry, d_hid.astype(jnp.bfloat16)

    init_carry = (
        jnp.zeros((VOCAB_SIZE, MODEL_DIM), jnp.float32),
        jnp.zeros((VOCAB_SIZE, MODEL_DIM), jnp.float32),
        jnp.zeros((MODEL_DIM, 2 * MODEL_DIM), jnp.float32),
        jnp.zeros((MODEL_DIM,), jnp.float32),
        jnp.zeros((MODEL_DIM,), jnp.float32),
        jnp.zeros((MODEL_DIM,), jnp.float32),
        jnp.zeros((), jnp.float32),
    )
    final_carry, d_hid_blocks = lax.scan(block_step, init_carry, block_inputs)
    d_out, d_emb, d_proj, d_gain_h, d_gain_e, d_gain_f, loss_sum = final_carry
    loss = (MTP_WEIGHT * loss_sum / (BATCH_ROWS * (SEQ_LEN - 2))).reshape(1)
    d_hidden = d_hid_blocks.reshape(BATCH_ROWS, SEQ_LEN, MODEL_DIM)
    return (loss, d_hidden, d_proj, d_emb, d_out, d_gain_h, d_gain_e, d_gain_f)
```

```python
import functools

import jax
import jax.numpy as jnp
from jax import lax
from jax.experimental import pallas as pl
from jax.experimental.pallas import tpu as pltpu
from jax.sharding import PartitionSpec as P


MTP_WEIGHT = 0.3
NORM_EPS = 1e-6
LOG2E = 1.4426950408889634
LN2 = 0.6931471805599453
NEG = -1e30
V_TILE = 2096
N_CHUNK = 3
N_PART = 3
VMEM_BYTES = 67043328
f32, bf16 = jnp.float32, jnp.bfloat16
NT = (((1,), (1,)), ((), ()))
NN = (((1,), (0,)), ((), ()))
TN = (((0,), (0,)), ((), ()))
CORE_SWAP = [(0, 1), (1, 0), (2, 3), (3, 2)]
X_SWAP = [(0, 2), (2, 0), (1, 3), (3, 1)]
Y_SWAP = [(0, 1), (1, 0)]


def cuts(size, pieces, step):
    edges = [((size * i) // pieces) // step * step for i in range(pieces)] + [size]
    return list(zip(edges[:-1], edges[1:]))


def tree(op, items):
    items = list(items)
    while len(items) > 1:
        items = [op(items[i], items[i + 1]) if i + 1 < len(items) else items[i] for i in range(0, len(items), 2)]
    return items[0]


def alternate(first, second):
    out = []
    for i in range(max(len(first), len(second))):
        out += first[i:i + 1] + second[i:i + 1]
    return out


def interleave(dots, passes):
    done = 0
    for i, dot in enumerate(dots):
        dot()
        while done < len(passes) and (done + 1) * len(dots) <= (i + 1) * len(passes):
            passes[done]()
            done += 1
    for piece in passes[done:]:
        piece()


def grad_piece(y_ref, g_ref, lab_ref, le_ref, wt_ref, hit_ref, base, row0, lanes, scale, l, r0, r1):
    sl = pl.ds(pl.multiple_of(base + l, lanes), lanes)
    lab = lab_ref[:, sl] - (lax.broadcasted_iota(jnp.int32, (8, lanes), 0) + row0)
    le = jnp.broadcast_to(le_ref[:, sl], (8, lanes))
    wt = jnp.broadcast_to(wt_ref[:, sl], (8, lanes))
    if hit_ref is not None:
        acc = [hit_ref[:8, sl], hit_ref[8:, sl]]
    for r in range(r0, r1, 16):
        halves = []
        for q in (0, 8):
            y = y_ref[r + q:r + q + 8, l:l + lanes]
            if scale:
                y = y * LOG2E
            hit = lab == (r + q)
            e = jnp.exp2(y - le)
            halves.append(jnp.where(hit, e - wt, e))
            if hit_ref is not None:
                acc[q // 8] = jnp.where(hit, y, acc[q // 8])
        g_ref[r:r + 16, l:l + lanes] = jnp.concatenate(halves, axis=0).astype(bf16)
    if hit_ref is not None:
        hit_ref[:8, sl] = acc[0]
        hit_ref[8:, sl] = acc[1]


def once():
    return dict(pipeline_mode=pl.Buffered(1))


def params():
    return pltpu.CompilerParams(vmem_limit_bytes=VMEM_BYTES)


def cost(dots, rows, n, extra):
    return pl.CostEstimate(flops=2 * dots * rows * n * 512, bytes_accessed=extra, transcendentals=rows * n)


def rms_parts(x):
    return lax.rsqrt(jnp.mean(x * x, axis=-1, keepdims=True) + NORM_EPS)


def rms_back(dy, x, r, gain):
    dg = dy * gain
    dx = r * dg - x * (r * r * r) * jnp.mean(dg * x, axis=-1, keepdims=True)
    n, width = x.shape
    return dx, jnp.sum((dy * x * r).reshape(n // 8, 8, width), axis=0)


def mix(h_ref, own_ref, recv_ref, w_ref, g_ref):
    h = h_ref[...].astype(f32)
    e = own_ref[...] + recv_ref[...]
    rh, re = rms_parts(h), rms_parts(e)
    joined = jnp.concatenate([(h * rh * g_ref[0:1, :]).astype(bf16), (e * re * g_ref[1:2, :]).astype(bf16)], axis=1)
    mixed = lax.dot_general(joined, w_ref[...], NT, preferred_element_type=f32)
    return h, e, rh, re, joined, mixed, rms_parts(mixed)


def tiles_of(tile, *widths):
    return [pl.BlockSpec((tile, w), lambda i: (i, 0)) for w in widths]


def front_kernel(hid, own, recv, w_proj, gains):
    n, width = hid.shape
    tile = 512

    def body(h_ref, own_ref, recv_ref, w_ref, g_ref, out_ref):
        mixed, rf = mix(h_ref, own_ref, recv_ref, w_ref, g_ref)[5:]
        out_ref[...] = mixed * rf * g_ref[2:3, :]

    return pl.pallas_call(
        body,
        grid=(n // tile,),
        in_specs=tiles_of(tile, width, width, width) + [
            pl.BlockSpec((width, 2 * width), lambda i: (0, 0)), pl.BlockSpec((3, width), lambda i: (0, 0))],
        out_specs=tiles_of(tile, width)[0],
        out_shape=jax.ShapeDtypeStruct((n, width), f32),
        compiler_params=params(),
        cost_estimate=pl.CostEstimate(flops=4 * n * width * width, bytes_accessed=14 * n * width, transcendentals=3 * n),
        name="front",
    )(hid, own, recv, w_proj, gains)


def back_kernel(hid, own, recv, w_proj, gains, df_mine, df_recv, totals):
    n, width = hid.shape
    tile = 512

    def body(h_ref, own_ref, recv_ref, w_ref, g_ref, a_ref, b_ref, *rest):
        dh_ref, de_ref, dw_ref, dg_ref = rest[-4:]
        h, e, rh, re, joined, mixed, rf = mix(h_ref, own_ref, recv_ref, w_ref, g_ref)
        df = (a_ref[...] + b_ref[...]).T
        du, dgf = rms_back(df, mixed, rf, g_ref[2:3, :])
        du = du.astype(bf16)
        dx = lax.dot_general(du, w_ref[...], NN, preferred_element_type=f32)
        dh, dgh = rms_back(dx[:, :width], h, rh, g_ref[0:1, :])
        de, dge = rms_back(dx[:, width:], e, re, g_ref[1:2, :])
        dh_ref[...] = dh.astype(bf16)
        de_ref[...] = de
        dw = lax.dot_general(du, joined, TN, preferred_element_type=f32)

        @pl.when(pl.program_id(0) == 0)
        def _():
            dw_ref[...] = rest[0][...] if totals else jnp.zeros_like(dw_ref)
            dg_ref[...] = rest[1][...] if totals else jnp.zeros_like(dg_ref)

        dw_ref[...] += dw
        dg_ref[0:8, :] += dgh
        dg_ref[8:16, :] += dge
        dg_ref[16:24, :] += dgf

    cols = pl.BlockSpec((width, tile), lambda i: (0, i))
    sums = [pl.BlockSpec((width, 2 * width), lambda i: (0, 0)), pl.BlockSpec((24, width), lambda i: (0, 0))]
    return pl.pallas_call(
        body,
        grid=(n // tile,),
        in_specs=tiles_of(tile, width, width, width) + [
            pl.BlockSpec((width, 2 * width), lambda i: (0, 0)), pl.BlockSpec((3, width), lambda i: (0, 0)), cols, cols]
        + sums[:len(totals)],
        out_specs=tiles_of(tile, width, width) + sums,
        out_shape=[
            jax.ShapeDtypeStruct((n, width), bf16), jax.ShapeDtypeStruct((n, width), f32),
            jax.ShapeDtypeStruct((width, 2 * width), f32), jax.ShapeDtypeStruct((24, width), f32)],
        compiler_params=params(),
        cost_estimate=pl.CostEstimate(flops=12 * n * width * width, bytes_accessed=24 * n * width, transcendentals=3 * n),
        name="back",
    )(hid, own, recv, w_proj, gains, df_mine, df_recv, *totals)


def merge_stats(mine, other, swap_halves, wt):
    n = mine.shape[1]

    def body(a_ref, b_ref, *rest):
        m, s = a_ref[0:1, :], a_ref[1:2, :]
        if swap_halves:
            b = jnp.concatenate([b_ref[:, n // 2:], b_ref[:, :n // 2]], axis=1)
        else:
            b = b_ref[...]
        top = jnp.maximum(m, b[0:1, :])
        total = s * jnp.exp2(m - top) + b[1:2, :] * jnp.exp2(b[0:1, :] - top)
        if wt is None:
            rest[0][...] = jnp.concatenate([top, total], axis=0)
        else:
            lse = top + jnp.log2(total)
            rest[1][...] = lse
            rest[2][...] = lse - jnp.log2(rest[0][...])

    row = jax.ShapeDtypeStruct((1, n), f32)
    args = (mine, other) if wt is None else (mine, other, wt)
    return pl.pallas_call(
        body,
        out_shape=jax.ShapeDtypeStruct((2, n), f32) if wt is None else [row, row],
        name="merge_stats",
    )(*args)


def round_rows(parts):
    m, (n, width) = len(parts), parts[0].shape
    tile = 768
    steps = n // tile

    def body(*refs):
        k = pl.program_id(0)
        for i in range(m):
            @pl.when(k == i)
            def _(i=i):
                refs[m][...] = refs[i][...].astype(bf16)

    def spec(i):
        return pl.BlockSpec((tile, width), lambda k, b: (jnp.where(k == i, b, jnp.where(k > i, steps - 1, 0)), 0))

    return pl.pallas_call(
        body,
        grid=(m, steps),
        in_specs=[spec(i) for i in range(m)],
        out_specs=pl.BlockSpec((tile, width), lambda k, b: (k * steps + b, 0)),
        out_shape=jax.ShapeDtypeStruct((m * n, width), bf16),
        compiler_params=params(),
        name="round_rows",
    )(*parts)


def logits_kernel(core, out_tab, feats, rows):
    n = feats.shape[0]
    t, lanes, groups = 768, 256, 2
    nv, nj = rows // V_TILE, n // (2 * t)

    def stats(y_ref, m_ref, s_ref, start):
        for l in range(0, t, lanes):
            sl = pl.ds(pl.multiple_of(start + l, lanes), lanes)
            old = m_ref[:, sl]
            acc = [old] + [None] * (groups - 1)
            for i, r in enumerate(range(0, V_TILE, 8)):
                x = y_ref[r:r + 8, l:l + lanes]
                acc[i % groups] = x if acc[i % groups] is None else jnp.maximum(acc[i % groups], x)
            new = tree(jnp.maximum, acc)
            acc = [s_ref[:, sl] * jnp.exp2(old - new)] + [None] * (groups - 1)
            for i, r in enumerate(range(0, V_TILE, 8)):
                x = jnp.exp2(y_ref[r:r + 8, l:l + lanes] - new)
                acc[i % groups] = x if acc[i % groups] is None else acc[i % groups] + x
            s_ref[:, sl] = tree(jnp.add, acc)
            m_ref[:, sl] = new

    def body(core_ref, w_ref, f_ref, y_ref, st_ref, ya, yb, m_ref, s_ref):
        v, j = pl.program_id(0), pl.program_id(1)
        step = v * nj + j

        @pl.when(step == 0)
        def _():
            m_ref[...] = jnp.full_like(m_ref, NEG)
            s_ref[...] = jnp.zeros_like(s_ref)
            yb[...] = jnp.full_like(yb, 2 * NEG)

        base = pl.multiple_of(j * 2 * t, 2 * t)
        prev = pl.multiple_of(lax.rem(j + nj - 1, nj) * 2 * t, 2 * t)
        w = w_ref[...]

        def dot(start, buf, lo):
            y = lax.dot_general(w, f_ref[pl.ds(start, t), :], NT, preferred_element_type=f32) * LOG2E
            buf[...] = y
            y_ref[:, lo:lo + t] = y

        dot(base, ya, 0)
        stats(yb, m_ref, s_ref, prev + t)
        dot(base + t, yb, t)
        stats(ya, m_ref, s_ref, base)

        @pl.when(step == nv * nj - 1)
        def _():
            stats(yb, m_ref, s_ref, base + t)
            m = m_ref[...]
            top = jnp.max(m, axis=0, keepdims=True)
            st_ref[0:1, :] = top
            st_ref[1:2, :] = jnp.sum(s_ref[...] * jnp.exp2(m - top), axis=0, keepdims=True)

    grid_spec = pltpu.PrefetchScalarGridSpec(
        num_scalar_prefetch=1,
        grid=(nv, nj),
        in_specs=[
            pl.BlockSpec((V_TILE, 512), lambda v, j, c: (c[0] * nv + v, 0)),
            pl.BlockSpec((n, 512), lambda v, j, c: (0, 0), **once()),
        ],
        out_specs=[pl.BlockSpec((V_TILE, 2 * t), lambda v, j, c: (v, j)), pl.BlockSpec((2, n), lambda v, j, c: (0, 0))],
        scratch_shapes=[pltpu.VMEM((V_TILE, t), f32)] * 2 + [pltpu.VMEM((8, n), f32)] * 2,
    )
    return pl.pallas_call(
        body,
        grid_spec=grid_spec,
        out_shape=[jax.ShapeDtypeStruct((rows, n), f32), jax.ShapeDtypeStruct((2, n), f32)],
        compiler_params=params(),
        cost_estimate=cost(1, rows, n, 4 * rows * n),
        name="logits",
    )(core, out_tab, feats)


def own_kernel(core, logits, feats, out_tab, lab, le, wt, acc):
    rows, n = logits.shape
    t, lanes, pm, pn, pr = 768, 256, 12, 256, 8
    nv, nj = rows // V_TILE, n // t
    last = nv * nj

    def body(core_ref, y_ref, f_ref, w_ref, lab_ref, le_ref, wt_ref, *rest):
        if acc is not None:
            in_ref, dw_ref, dfa_ref, dfb_ref, hit_ref, ga, gb, df_ref = rest
        else:
            dw_ref, dfa_ref, dfb_ref, hit_ref, ga, gb, df_ref = rest
        s = pl.program_id(0)
        v, j, pj = s // nj, lax.rem(s, nj), lax.rem(s - 1 + nj, nj)
        base, prev = pl.multiple_of(j * t, t), pl.multiple_of(pj * t, t)
        half = pj // (nj // 2)
        half_start = (pj - half * (nj // 2)) * t

        @pl.when(s == 0)
        def _():
            df_ref[...] = jnp.zeros_like(df_ref)
            hit_ref[...] = jnp.zeros_like(hit_ref)

        @pl.when((pj == 0) & (s > 0))
        def _():
            dw_ref[...] = jnp.zeros_like(dw_ref) if acc is None else in_ref[...]

        def grads(g):
            return [
                functools.partial(grad_piece, y_ref, g, lab_ref, le_ref, wt_ref, hit_ref, base, v * V_TILE, lanes, False, l, r0, r1)
                for l in range(0, t, lanes) for r0, r1 in cuts(V_TILE, pr, 16)
            ]

        def dots(g):
            def out_piece(r0, r1):
                dw_ref[r0:r1, :] += lax.dot_general(g[r0:r1, :], f_ref[pl.ds(prev, t), :], NN, preferred_element_type=f32)

            def feat_piece(l):
                sl = pl.ds(pl.multiple_of(half_start + l, pn), pn)
                df_ref[half, :, sl] += lax.dot_general(w_ref[...], g[:, l:l + pn], TN, preferred_element_type=f32)

            return alternate(
                [functools.partial(out_piece, r0, r1) for r0, r1 in cuts(V_TILE, pm, 16)],
                [functools.partial(feat_piece, l) for l in range(0, t, pn)],
            )

        odd = lax.rem(s, 2) == 1

        @pl.when(s == 0)
        def _():
            interleave([], grads(ga))

        @pl.when((s > 0) & (s < last) & odd)
        def _():
            interleave(dots(ga), grads(gb))

        @pl.when((s > 0) & (s < last) & jnp.logical_not(odd))
        def _():
            interleave(dots(gb), grads(ga))

        @pl.when(s == last)
        def _():
            interleave(dots(ga if last % 2 == 1 else gb), [])
            dfa_ref[...] = df_ref[0]
            dfb_ref[...] = df_ref[1]

    def now(s):
        return jnp.minimum(s, last - 1)

    def lag(s):
        return jnp.maximum(s - 1, 0) // nj

    row = pl.BlockSpec((1, n), lambda s, c: (0, 0), **once())
    in_specs = [
        pl.BlockSpec((V_TILE, t), lambda s, c: (now(s) // nj, lax.rem(now(s), nj))),
        pl.BlockSpec((n, 512), lambda s, c: (0, 0), **once()),
        pl.BlockSpec((V_TILE, 512), lambda s, c: (c[0] * nv + lag(s), 0)),
        row, row, row,
    ]
    args = [logits, feats, out_tab, lab, le, wt]
    if acc is not None:
        in_specs.append(pl.BlockSpec((V_TILE, 512), lambda s, c: (lag(s), 0)))
        args.append(acc)
    grid_spec = pltpu.PrefetchScalarGridSpec(
        num_scalar_prefetch=1,
        grid=(last + 1,),
        in_specs=in_specs,
        out_specs=[
            pl.BlockSpec((V_TILE, 512), lambda s, c: (lag(s), 0)),
            pl.BlockSpec((512, n // 2), lambda s, c: (0, 0), **once()),
            pl.BlockSpec((512, n // 2), lambda s, c: (0, 0), **once()),
            pl.BlockSpec((16, n), lambda s, c: (0, 0), **once()),
        ],
        scratch_shapes=[pltpu.VMEM((V_TILE, t), bf16)] * 2 + [pltpu.VMEM((2, 512, n // 2), f32)],
    )
    return pl.pallas_call(
        body,
        grid_spec=grid_spec,
        out_shape=[
            jax.ShapeDtypeStruct((rows, 512), f32), jax.ShapeDtypeStruct((512, n // 2), f32),
            jax.ShapeDtypeStruct((512, n // 2), f32), jax.ShapeDtypeStruct((16, n), f32)],
        input_output_aliases={7: 0} if acc is not None else {},
        compiler_params=params(),
        cost_estimate=cost(2, rows, n, 4 * rows * n),
        name="own",
    )(core, *args)


def other_kernel(core, feats, out_tab, lab, le, wt, acc, whole, part):
    n = feats.shape[0]
    rows = acc.shape[0]
    t, lanes, pz, pm, pr = 768, 256, 6, 6, 4
    nv_all = rows // V_TILE
    nv, nj = nv_all // N_PART, n // t
    v0 = part * nv
    last = nv * nj

    def body(core_ref, f_ref, w_ref, lab_ref, le_ref, wt_ref, in_ref, *rest):
        if whole is not None:
            rest = rest[1:]
        part_ref, dw_ref, ya, yb, ga, gb = rest
        s = pl.program_id(0)

        def start(k):
            return pl.multiple_of(lax.rem(s - k + 2 * nj, nj) * t, t)

        b0, b1, b2 = start(0), start(1), start(2)
        row0 = jnp.where(s >= 1, (v0 + (s - 1) // nj) * V_TILE, 1 << 24)

        @pl.when(s == 0)
        def _():
            yb[...] = jnp.full_like(yb, NEG)
            ga[...] = jnp.zeros_like(ga)
            gb[...] = jnp.zeros_like(gb)

        @pl.when((b2 == 0) & (s > 1))
        def _():
            dw_ref[...] = in_ref[...]

        def step(y_new, y_old, g_new, g_old):
            def logit_piece(r0, r1):
                y_new[r0:r1, :] = lax.dot_general(w_ref[r0:r1, :], f_ref[pl.ds(b0, t), :], NT, preferred_element_type=f32)

            def out_piece(r0, r1):
                dw_ref[r0:r1, :] += lax.dot_general(g_old[r0:r1, :], f_ref[pl.ds(b2, t), :], NN, preferred_element_type=f32)

            dots = alternate(
                [functools.partial(logit_piece, r0, r1) for r0, r1 in cuts(V_TILE, pz, 16)],
                [functools.partial(out_piece, r0, r1) for r0, r1 in cuts(V_TILE, pm, 16)],
            )
            grads = [
                functools.partial(grad_piece, y_old, g_new, lab_ref, le_ref, wt_ref, None, b1, row0, lanes, True, l, r0, r1)
                for l in range(0, t, lanes) for r0, r1 in cuts(V_TILE, pr, 16)
            ]
            interleave(dots, grads)

        odd = lax.rem(s, 2) == 1

        @pl.when(odd)
        def _():
            step(yb, ya, ga, gb)

        @pl.when(jnp.logical_not(odd))
        def _():
            step(ya, yb, gb, ga)

        @pl.when((lax.rem(s - 2 + nj, nj) == nj - 1) & (s > 1))
        def _():
            part_ref[...] = dw_ref[...]

    def now(s):
        return v0 + jnp.minimum(s, last - 1) // nj

    def lag(s):
        return jnp.maximum(s - 2, 0) // nj

    row = pl.BlockSpec((1, n), lambda s, c: (0, 0), **once())
    in_specs = [
        pl.BlockSpec((n, 512), lambda s, c: (0, 0), **once()),
        pl.BlockSpec((V_TILE, 512), lambda s, c: (c[0] * nv_all + now(s), 0)),
        row, row, row,
        pl.BlockSpec((V_TILE, 512), lambda s, c: (v0 + lag(s), 0)),
    ]
    args = [feats, out_tab, lab, le, wt, acc]
    if whole is not None:
        in_specs.append(pl.BlockSpec(memory_space=pl.ANY))
        args.append(whole)
    grid_spec = pltpu.PrefetchScalarGridSpec(
        num_scalar_prefetch=1,
        grid=(last + 2,),
        in_specs=in_specs,
        out_specs=[
            pl.BlockSpec((V_TILE, 512), lambda s, c: (lag(s), 0)),
            pl.BlockSpec((V_TILE, 512), lambda s, c: (c[0] * nv_all + v0 + lag(s), 0)),
        ],
        scratch_shapes=[pltpu.VMEM((V_TILE, t), f32)] * 2 + [pltpu.VMEM((V_TILE, t), bf16)] * 2,
    )
    return pl.pallas_call(
        body,
        grid_spec=grid_spec,
        out_shape=[jax.ShapeDtypeStruct((nv * V_TILE, 512), f32), jax.ShapeDtypeStruct((2 * rows, 512), f32)],
        input_output_aliases={7: 1} if whole is not None else {},
        compiler_params=params(),
        cost_estimate=cost(2, nv * V_TILE, n, 12 * nv * V_TILE * 512),
        name="other",
    )(core, *args)


def row_sums(order, ids, bounds, parts, block):
    m, (n, width) = len(parts), parts[0].shape
    unroll = 16

    def body(order_ref, id_ref, b_ref, *rest):
        ins, (out_ref, buf, sem) = rest[:m], rest[m:]
        p = pl.program_id(0)

        def fetch(i):
            return pltpu.make_async_copy(ins[i], buf.at[pl.ds(i * n, n)], sem.at[i])

        @pl.when(p == 0)
        def _():
            for i in range(m):
                fetch(i).start()

        out_ref[...] = jnp.zeros_like(out_ref)

        @pl.when(p == 0)
        def _():
            for i in range(m):
                fetch(i).wait()

        lo, hi = b_ref[p], b_ref[p + 1]

        def one(k, carry):
            prev, acc = carry
            row, d = order_ref[k], id_ref[k]
            x = buf[pl.ds(row, 1), :]
            acc = jnp.where(d == prev, acc + x, x)
            out_ref[pl.ds(d - p * V_TILE, 1), :] = acc
            return d, acc

        def several(i, carry):
            for u in range(unroll):
                carry = one(lo + i * unroll + u, carry)
            return carry

        full = (hi - lo) // unroll
        carry = lax.fori_loop(0, full, several, (jnp.int32(-1), jnp.zeros((1, width), f32)))
        lax.fori_loop(lo + full * unroll, hi, one, carry)

    grid_spec = pltpu.PrefetchScalarGridSpec(
        num_scalar_prefetch=3,
        grid=(block // V_TILE,),
        in_specs=[pl.BlockSpec(memory_space=pl.ANY)] * m,
        out_specs=pl.BlockSpec((V_TILE, width), lambda p, *_: (p, 0)),
        scratch_shapes=[pltpu.VMEM((m * n, width), f32), pltpu.SemaphoreType.DMA((m,))],
    )
    return pl.pallas_call(
        body,
        grid_spec=grid_spec,
        out_shape=jax.ShapeDtypeStruct((block, width), f32),
        compiler_params=params(),
        cost_estimate=pl.CostEstimate(flops=150_000_000, bytes_accessed=4 * (m * n + block) * width, transcendentals=0),
        name="row_sums",
    )(order, ids, bounds, *parts)


def solution(mesh):
    def local_step(hidden, tokens, emb_blk, out_blk, w_proj, gain_h, gain_e, gain_f):
        batch, piece, width = hidden.shape
        block = emb_blk.shape[0]
        rows = block // 2
        n_own = batch * piece
        n_c = n_own // N_CHUNK
        tp_rank, cp_rank = lax.axis_index("tp"), lax.axis_index("cp")
        core = lax.rem(cp_rank, 2)
        core_arg = core.reshape(1)
        seq_len = piece * 4
        row_start = tp_rank * block + core * rows

        def core_swap(v):
            return lax.ppermute(v, "cp", CORE_SWAP)

        def x_swap(v):
            return lax.ppermute(v, "cp", X_SWAP)

        def y_swap(v):
            return lax.ppermute(v, "tp", Y_SWAP)

        def weight_of(rank):
            pos = rank * piece + jnp.arange(piece)
            return jnp.broadcast_to(MTP_WEIGHT * (pos < seq_len - 2).astype(f32), (batch, piece)).reshape(N_CHUNK, n_c)

        head = lax.ppermute(tokens[:, :2], "cp", [(k + 1, k) for k in range(3)])
        ahead = jnp.concatenate([tokens, head], axis=1)
        ids_own = jnp.stack([ahead[:, 1:piece + 1], ahead[:, 2:]]).reshape(2, N_CHUNK, n_c)
        ids_mate = core_swap(ids_own)
        ids_far = x_swap(ids_own)
        ids_diag = core_swap(ids_far)
        next_ids = [v[0] for v in (ids_own, ids_mate, ids_far, ids_diag)]
        labels = [v[1] - row_start for v in (ids_own, ids_mate, ids_far, ids_diag)]
        weights = [weight_of(cp_rank ^ k) for k in range(4)]

        local_next = next_ids[0] - tp_rank * block
        in_block = (local_next >= 0) & (local_next < block)
        take = jnp.clip(local_next, 0, block - 1)
        hid = hidden.reshape(N_CHUNK, n_c, width)

        emb_own, emb_recv = [], []
        for c in range(N_CHUNK):
            e = jnp.where(in_block[c][:, None], jnp.take(emb_blk, take[c], axis=0).astype(f32), 0.0)
            emb_own.append(e)
            emb_recv.append(y_swap(e))

        ids_all = jnp.concatenate([next_ids[k].reshape(-1) for k in (0, 2, 1, 3)]) - tp_rank * block
        seg = jnp.where((ids_all >= 0) & (ids_all < block), ids_all, block)
        seg_sorted, order = lax.sort((seg, jnp.arange(4 * n_own, dtype=jnp.int32)), num_keys=1)
        starts = jnp.arange(block // V_TILE + 1) * V_TILE
        bounds = jnp.sum(seg[None, :] < starts[:, None], axis=1).astype(jnp.int32)

        gains = jnp.stack([gain_h, gain_e, gain_f])
        f_pair, far_parts, logits, stats = [], [], [], []
        for c in range(N_CHUNK):
            normed = front_kernel(hid[c], emb_own[c], emb_recv[c], w_proj, gains)
            mate = core_swap(normed)
            f_pair.append(round_rows([normed, mate]))
            far = x_swap(normed)
            far_parts += [far, core_swap(far)]
            y, st = logits_kernel(core_arg, out_blk, f_pair[c], rows)
            logits.append(y)
            stats.append(st)

        le_pair, le_far, lse_own, wt_pair = [], [], [], []
        for c in range(N_CHUNK):
            recv = core_swap(stats[c])
            both = merge_stats(stats[c], recv, True, None)
            recv = y_swap(both)
            wt_pair.append(jnp.concatenate([weights[0][c], weights[1][c]])[None])
            lse, le = merge_stats(both, recv, False, wt_pair[c])
            lse_own.append(lse[0, :n_c])
            le_pair.append(le)
            le_far.append(x_swap(le))

        acc, df_terms, hits = None, [], []
        for c in range(N_CHUNK):
            lab = jnp.concatenate([labels[0][c], labels[1][c]])
            acc, df_own, df_mate, hit = own_kernel(core_arg, logits[c], f_pair[c], out_blk, lab[None], le_pair[c], wt_pair[c], acc)
            recv = core_swap(df_mate)
            mine = df_own + recv
            recv = y_swap(mine)
            df_terms.append((mine, recv))
            hits.append(hit)

        f_far = round_rows(far_parts)
        lab_far = jnp.concatenate([labels[k][c] for c in range(N_CHUNK) for k in (2, 3)])
        wt_far = jnp.concatenate([weights[k][c] for c in range(N_CHUNK) for k in (2, 3)])
        whole, mates = None, []
        for part in range(N_PART):
            piece_out, whole = other_kernel(core_arg, f_far, out_blk, lab_far[None], jnp.concatenate(le_far, axis=1), wt_far[None], acc, whole, part)
            mates.append(core_swap(piece_out))

        d_hid, totals, de_own, de_far, de_mate, de_diag = [], (), [], [], [], []
        for c in range(N_CHUNK):
            dh, de, *totals = back_kernel(hid[c], emb_own[c], emb_recv[c], w_proj, gains, *df_terms[c], totals)
            d_hid.append(dh)
            de_own.append(de)
            de_far.append(x_swap(de))
            de_mate.append(core_swap(de))
            de_diag.append(core_swap(de_far[c]))

        loss_part = 0.5 * jnp.sum(weights[0] * jnp.stack(lse_own)) - sum(jnp.sum(w * h) for w, h in zip(wt_pair, hits))
        d_proj = totals[0]
        small = jnp.concatenate([jnp.sum(totals[1].reshape(3, 8, width), axis=1), jnp.full((5, width), loss_part)], axis=0)
        d_proj, small = d_proj + core_swap(d_proj), small + core_swap(small)
        d_proj, small = d_proj + x_swap(d_proj), small + x_swap(small)
        loss_sum = small[3:4, 0] + y_swap(small[3:, :128])[0:1, 0]

        d_emb = row_sums(order, seg_sorted, bounds, de_own + de_far + de_mate + de_diag, block)

        for part in range(N_PART):
            start = (1 - core) * rows + part * (rows // N_PART)
            whole = lax.dynamic_update_slice(whole, mates[part], (start, 0))

        loss = LN2 * loss_sum / (batch * (seq_len - 2))
        d_hidden = jnp.concatenate(d_hid, axis=0).reshape(batch, piece, width)
        return loss, d_hidden, d_proj, d_emb, whole, small[0], small[1], small[2]

    part_seq = P("dp", "cp", None)
    in_specs = (part_seq, P("dp", "cp"), P("tp", None), P("tp", None), P(None, None), P(None), P(None), P(None))
    out_specs = (P("dp"), part_seq, P("dp", None), P(("dp", "tp"), None), P(("dp", "tp"), None), P("dp"), P("dp"), P("dp"))
    return jax.shard_map(local_step, mesh=mesh, in_specs=in_specs, out_specs=out_specs, check_vma=False)
```

```python
import functools

import jax
import jax.numpy as jnp
from jax import lax
from jax.experimental import pallas as pl
from jax.experimental.pallas import tpu as pltpu
from jax.sharding import PartitionSpec as P


MTP_WEIGHT = 0.3
NORM_EPS = 1e-6
LOG2E = 1.4426950408889634
LN2 = 0.6931471805599453
NEG = -1e30
V_TILE = 2096
N_CHUNK = 3
VMEM_BYTES = 67043328
f32, bf16 = jnp.float32, jnp.bfloat16
ALL, ORIGIN, WIDTH, STEP, LANES, PACK, SUB, TWO = Ellipsis, (0, 0), 512, 768, 256, 16, 8, 2
NT = (((1,), (1,)), ((), ()))
NN = (((1,), (0,)), ((), ()))
TN = (((0,), (0,)), ((), ()))
CORE_SWAP = [(0, 1), (1, 0), (2, 3), (3, 2)]
X_SWAP = [(0, 2), (2, 0), (1, 3), (3, 1)]
Y_SWAP = [(0, 1), (1, 0)]


def cuts(size, pieces, step):
    edges = [((size * i) // pieces) // step * step for i in range(pieces)] + [size]
    return list(zip(edges[:-1], edges[1:]))


def tree(op, items):
    items = list(items)
    while len(items) > 1:
        items = [op(items[i], items[i + 1]) if i + 1 < len(items) else items[i] for i in range(0, len(items), 2)]
    return items[0]


def alternate(first, second):
    out = []
    for i in range(max(len(first), len(second))):
        out += first[i:i + 1] + second[i:i + 1]
    return out


def interleave(dots, passes):
    done = 0
    for i, dot in enumerate(dots):
        dot()
        while done < len(passes) and (done + 1) * len(dots) <= (i + 1) * len(passes):
            passes[done]()
            done += 1
    for piece in passes[done:]:
        piece()


def grad_piece(y_ref, g_ref, lab_ref, le_ref, wt_ref, hit_ref, base, row0, lanes, scale, l, r0, r1):
    sl = pl.ds(pl.multiple_of(base + l, lanes), lanes)
    lab = lab_ref[:, sl] - (lax.broadcasted_iota(jnp.int32, (SUB, lanes), 0) + row0)
    le = jnp.broadcast_to(le_ref[:, sl], (SUB, lanes))
    wt = jnp.broadcast_to(wt_ref[:, sl], (SUB, lanes))
    if hit_ref is not None:
        acc = [hit_ref[:SUB, sl], hit_ref[SUB:, sl]]
    for r in range(r0, r1, PACK):
        halves = []
        for q in (0, SUB):
            y = y_ref[r + q:r + q + SUB, l:l + lanes]
            if scale:
                y = y * LOG2E
            hit = lab == (r + q)
            e = jnp.exp2(y - le)
            halves.append(jnp.where(hit, e - wt, e))
            if hit_ref is not None:
                acc[q // SUB] = jnp.where(hit, y, acc[q // SUB])
        g_ref[r:r + PACK, l:l + lanes] = jnp.concatenate(halves, axis=0).astype(bf16)
    if hit_ref is not None:
        hit_ref[:SUB, sl] = acc[0]
        hit_ref[SUB:, sl] = acc[1]


def once():
    return {}


def params():
    return pltpu.CompilerParams(vmem_limit_bytes=VMEM_BYTES)


def cost(dots, rows, n, extra):
    return pl.CostEstimate(flops=TWO * dots * rows * n * WIDTH, bytes_accessed=extra, transcendentals=rows * n)


def rms_parts(x):
    return lax.rsqrt(jnp.mean(x * x, axis=-1, keepdims=True) + NORM_EPS)


def rms_back(dy, x, r, gain):
    dg = dy * gain
    dx = r * dg - x * (r * r * r) * jnp.mean(dg * x, axis=-1, keepdims=True)
    n, width = x.shape
    return dx, jnp.sum((dy * x * r).reshape(n // SUB, SUB, width), axis=0)


def mix(h_ref, own_ref, recv_ref, w_ref, g_ref):
    h = h_ref[ALL].astype(f32)
    e = own_ref[ALL] + recv_ref[ALL]
    rh, re = rms_parts(h), rms_parts(e)
    joined = jnp.concatenate([(h * rh * g_ref[0:1, :]).astype(bf16), (e * re * g_ref[1:2, :]).astype(bf16)], axis=1)
    mixed = lax.dot_general(joined, w_ref[ALL], NT, preferred_element_type=f32)
    return h, e, rh, re, joined, mixed, rms_parts(mixed)


def tiles_of(tile, *widths):
    return [pl.BlockSpec((tile, w), lambda i: (i, 0)) for w in widths]


def front_kernel(hid, own, recv, w_proj, gains):
    n, width = hid.shape
    tile = WIDTH

    def body(h_ref, own_ref, recv_ref, w_ref, g_ref, out_ref):
        mixed, rf = mix(h_ref, own_ref, recv_ref, w_ref, g_ref)[5:]
        out_ref[ALL] = mixed * rf * g_ref[2:3, :]

    return pl.pallas_call(
        body,
        grid=(n // tile,),
        in_specs=tiles_of(tile, width, width, width) + [
            pl.BlockSpec((width, TWO * width), lambda i: ORIGIN), pl.BlockSpec((3, width), lambda i: ORIGIN)],
        out_specs=tiles_of(tile, width)[0],
        out_shape=jax.ShapeDtypeStruct((n, width), f32),
        compiler_params=params(),
        cost_estimate=pl.CostEstimate(flops=4 * n * width * width, bytes_accessed=14 * n * width, transcendentals=3 * n),
        name="front",
    )(hid, own, recv, w_proj, gains)


def back_kernel(hid, own, recv, w_proj, gains, df_mine, df_recv, chunk, totals):
    n, width = hid.shape
    tile = WIDTH

    def body(h_ref, own_ref, recv_ref, w_ref, g_ref, a_ref, b_ref, *rest):
        dh_ref, de_ref, dw_ref, dg_ref = rest[-4:]
        h, e, rh, re, joined, mixed, rf = mix(h_ref, own_ref, recv_ref, w_ref, g_ref)
        df = (a_ref[ALL] + b_ref[ALL]).T
        du, dgf = rms_back(df, mixed, rf, g_ref[2:3, :])
        du = du.astype(bf16)
        dx = lax.dot_general(du, w_ref[ALL], NN, preferred_element_type=f32)
        dh, dgh = rms_back(dx[:, :width], h, rh, g_ref[0:1, :])
        de, dge = rms_back(dx[:, width:], e, re, g_ref[1:2, :])
        dh_ref[ALL] = dh.astype(bf16)
        de_ref[ALL] = de
        dw = lax.dot_general(du, joined, TN, preferred_element_type=f32)

        @pl.when(pl.program_id(0) == 0)
        def _():
            dw_ref[ALL] = rest[0][ALL] if totals else jnp.zeros_like(dw_ref)
            dg_ref[ALL] = rest[1][ALL] if totals else jnp.zeros_like(dg_ref)

        dw_ref[ALL] += dw
        dg_ref[0:SUB, :] += dgh
        dg_ref[SUB:PACK, :] += dge
        dg_ref[PACK:24, :] += dgf

    cols = pl.BlockSpec((width, tile), lambda i: (0, i))
    sums = [pl.BlockSpec((width, TWO * width), lambda i: ORIGIN), pl.BlockSpec((24, width), lambda i: ORIGIN)]
    return pl.pallas_call(
        body,
        grid=(n // tile,),
        in_specs=tiles_of(tile, width, width, width) + [
            pl.BlockSpec((width, TWO * width), lambda i: ORIGIN), pl.BlockSpec((3, width), lambda i: ORIGIN), cols, cols]
        + (sums + [pl.BlockSpec(memory_space=pl.ANY)])[:len(totals)],
        input_output_aliases={9: 0} if totals else {},
        out_specs=[pl.BlockSpec((tile, width), lambda i: (chunk * (n // tile) + i, 0))] + tiles_of(tile, width) + sums,
        out_shape=[
            jax.ShapeDtypeStruct((N_CHUNK * n, width), bf16), jax.ShapeDtypeStruct((n, width), f32),
            jax.ShapeDtypeStruct((width, TWO * width), f32), jax.ShapeDtypeStruct((24, width), f32)],
        compiler_params=params(),
        cost_estimate=pl.CostEstimate(flops=12 * n * width * width, bytes_accessed=24 * n * width, transcendentals=3 * n),
        name="back",
    )(hid, own, recv, w_proj, gains, df_mine, df_recv, *totals)


def merge_halves(mine, mate):
    n = mine.shape[1]

    def body(a_ref, b_ref, out_ref):
        b = jnp.concatenate([b_ref[:, n // TWO:], b_ref[:, :n // TWO]], axis=1)
        out_ref[ALL] = merged(a_ref[ALL], b)

    return pl.pallas_call(body, out_shape=jax.ShapeDtypeStruct((2, n), f32), name="merge_halves")(mine, mate)


def merged(a, b):
    top = jnp.maximum(a[0:1, :], b[0:1, :])
    total = a[1:2, :] * jnp.exp2(a[0:1, :] - top) + b[1:2, :] * jnp.exp2(b[0:1, :] - top)
    return jnp.concatenate([top, total], axis=0)


def finish_stats(mine, other, wt, chunk, into):
    n = mine.shape[1]

    def body(a_ref, b_ref, wt_ref, *rest):
        both = merged(a_ref[ALL], b_ref[ALL])
        lse = both[0:1, :] + jnp.log2(both[1:2, :])
        rest[-2][ALL] = lse
        rest[-1][ALL] = lse - jnp.log2(wt_ref[ALL])

    here = pl.BlockSpec((1, n), lambda i: (0, chunk))
    block = pl.BlockSpec((2, n), lambda i: ORIGIN)
    return pl.pallas_call(
        body,
        grid=(1,),
        in_specs=[block, block, here] + [pl.BlockSpec(memory_space=pl.ANY)] * len(into),
        out_specs=[here, here],
        out_shape=[jax.ShapeDtypeStruct((1, N_CHUNK * n), f32)] * TWO,
        input_output_aliases={3: 0, 4: 1} if into else {},
        name="finish_stats",
    )(mine, other, wt, *into)


def round_rows(parts, total=None, slot=0, into=None):
    m, (n, width) = len(parts), parts[0].shape
    tile = STEP
    steps = n // tile
    total = m * n if total is None else total
    first = slot * m * steps

    def body(*refs):
        k = pl.program_id(0)
        for i in range(m):
            @pl.when(k == i)
            def _(i=i):
                refs[-1][ALL] = refs[i][ALL].astype(bf16)

    def spec(i):
        return pl.BlockSpec((tile, width), lambda k, b: (jnp.where(k == i, b, jnp.where(k > i, steps - 1, 0)), 0))

    extra = [] if into is None else [into]
    return pl.pallas_call(
        body,
        grid=(m, steps),
        in_specs=[spec(i) for i in range(m)] + [pl.BlockSpec(memory_space=pl.ANY)] * len(extra),
        out_specs=pl.BlockSpec((tile, width), lambda k, b: (first + k * steps + b, 0)),
        out_shape=jax.ShapeDtypeStruct((total, width), bf16),
        input_output_aliases={m: 0} if extra else {},
        compiler_params=params(),
        name="round_rows",
    )(*parts, *extra)


def logits_kernel(meta, out_tab, feats, rows, chunk, into):
    n = feats.shape[0] // N_CHUNK
    t, lanes, groups = STEP, LANES, 2
    nv, nj = rows // V_TILE, n // (TWO * t)
    extra = [] if into is None else [into]

    def stats(y_ref, m_ref, s_ref, start):
        for l in range(0, t, lanes):
            sl = pl.ds(pl.multiple_of(start + l, lanes), lanes)
            old = m_ref[:, sl]
            acc = [old] + [None] * (groups - 1)
            for i, r in enumerate(range(0, V_TILE, SUB)):
                x = y_ref[r:r + SUB, l:l + lanes]
                acc[i % groups] = x if acc[i % groups] is None else jnp.maximum(acc[i % groups], x)
            new = tree(jnp.maximum, acc)
            acc = [s_ref[:, sl] * jnp.exp2(old - new)] + [None] * (groups - 1)
            for i, r in enumerate(range(0, V_TILE, SUB)):
                x = jnp.exp2(y_ref[r:r + SUB, l:l + lanes] - new)
                acc[i % groups] = x if acc[i % groups] is None else acc[i % groups] + x
            s_ref[:, sl] = tree(jnp.add, acc)
            m_ref[:, sl] = new

    def body(meta_ref, w_ref, f_ref, *rest):
        y_ref, st_ref, ya, yb, m_ref, s_ref = rest[-6:]
        v, j = pl.program_id(0), pl.program_id(1)
        step = v * nj + j

        @pl.when(step == 0)
        def _():
            m_ref[ALL] = jnp.full_like(m_ref, NEG)
            s_ref[ALL] = jnp.zeros_like(s_ref)
            yb[ALL] = jnp.full_like(yb, TWO * NEG)

        base = pl.multiple_of(j * TWO * t, TWO * t)
        prev = pl.multiple_of(lax.rem(j + nj - 1, nj) * TWO * t, TWO * t)
        w = w_ref[ALL]

        def dot(start, buf, lo):
            y = lax.dot_general(w, f_ref[pl.ds(start, t), :], NT, preferred_element_type=f32) * LOG2E
            buf[ALL] = y
            y_ref[:, lo:lo + t] = y

        dot(base, ya, 0)
        stats(yb, m_ref, s_ref, prev + t)
        dot(base + t, yb, t)
        stats(ya, m_ref, s_ref, base)

        @pl.when(step == nv * nj - 1)
        def _():
            stats(yb, m_ref, s_ref, base + t)
            m = m_ref[ALL]
            top = jnp.max(m, axis=0, keepdims=True)
            st_ref[0:1, :] = top
            st_ref[1:2, :] = jnp.sum(s_ref[ALL] * jnp.exp2(m - top), axis=0, keepdims=True)

    grid_spec = pltpu.PrefetchScalarGridSpec(
        num_scalar_prefetch=1,
        grid=(nv, nj),
        in_specs=[
            pl.BlockSpec((V_TILE, WIDTH), lambda v, j, c: (c[0] * nv + v, 0)),
            pl.BlockSpec((n, WIDTH), lambda v, j, c: (chunk, 0), **once()),
        ] + [pl.BlockSpec(memory_space=pl.ANY)] * len(extra),
        out_specs=[pl.BlockSpec((V_TILE, TWO * t), lambda v, j, c: (v, chunk * nj + j)), pl.BlockSpec((2, n), lambda v, j, c: ORIGIN)],
        scratch_shapes=[pltpu.VMEM((V_TILE, t), f32)] * TWO + [pltpu.VMEM((SUB, n), f32)] * TWO,
    )
    return pl.pallas_call(
        body,
        grid_spec=grid_spec,
        out_shape=[jax.ShapeDtypeStruct((rows, N_CHUNK * n), f32), jax.ShapeDtypeStruct((2, n), f32)],
        input_output_aliases={3: 0} if extra else {},
        compiler_params=params(),
        cost_estimate=cost(1, rows, n, 4 * rows * n),
        name="logits",
    )(meta, out_tab, feats, *extra)


def own_kernel(meta, logits, feats, out_tab, lab, le, wt, kept, chunk, d_feats, d_out):
    rows, n_all = logits.shape
    whole = chunk is None
    n = n_all if whole else n_all // N_CHUNK
    half_n = n_all // N_CHUNK // TWO
    t, lanes, pm, pn, pr = STEP, LANES, 12, LANES, SUB
    nv = rows // V_TILE
    nk = nv // TWO
    n_tiles, nj = (1 if whole else nk + 1), n // t
    per_half = half_n // t
    last = n_tiles * nj
    at = 0 if whole else chunk

    def tile(m, k):
        keep = nk * m[1] + kept
        return keep if whole else jnp.where(k < nk, nk * (1 - m[1]) + k, keep)

    def body(meta_ref, y_ref, f_ref, w_ref, lab_ref, le_ref, wt_ref, *rest):
        rest = list(rest)
        df_in = rest.pop(0) if d_feats is not None else None
        dw_in = rest.pop(0) if d_out is not None else None
        if whole:
            dw_ref, df_ref, hit_ref, ga, gb = rest
        else:
            dw_ref, dfa_ref, dfb_ref, hit_ref, ga, gb, df_ref, sem = rest
        s = pl.program_id(0)
        k, j, pk, pj = s // nj, lax.rem(s, nj), (s - 1) // nj, lax.rem(s - 1 + nj, nj)
        base = pl.multiple_of(j * t, t)
        row0 = tile(meta_ref, k) * V_TILE
        pjc = lax.rem(pj, TWO * per_half)
        half = pjc // per_half
        half_start = (pjc - half * per_half) * t

        def fetch():
            return pltpu.make_async_copy(df_in.at[chunk], df_ref, sem)

        if whole:
            @pl.when((s > 0) & (pjc == 0))
            def _():
                df_ref[ALL] = jnp.zeros_like(df_ref) if df_in is None else df_in[ALL]

        @pl.when(s == 0)
        def _():
            if not whole:
                fetch().start()
            hit_ref[ALL] = jnp.zeros_like(hit_ref)
            dw_ref[ALL] = jnp.zeros_like(dw_ref) if dw_in is None else dw_in[ALL]

        def grads(g):
            return [
                functools.partial(grad_piece, y_ref, g, lab_ref, le_ref, wt_ref, hit_ref, base, row0, lanes, False, l, r0, r1)
                for l in range(0, t, lanes) for r0, r1 in cuts(V_TILE, pr, PACK)
            ]

        def dots(g, with_out):
            def out_piece(r0, r1):
                dw_ref[r0:r1, :] += lax.dot_general(g[r0:r1, :], f_ref[ALL], NN, preferred_element_type=f32)

            def feat_piece(l, k0, k1):
                sl = pl.ds(pl.multiple_of(half_start + l, pn), pn)
                df_ref[half, :, sl] += lax.dot_general(w_ref[k0:k1, :], g[k0:k1, l:l + pn], TN, preferred_element_type=f32)

            out = [functools.partial(out_piece, r0, r1) for r0, r1 in cuts(V_TILE, pm, PACK)] if with_out else []
            pk = [(0, V_TILE)] if with_out else [(0, WIDTH), (WIDTH, 1024), (1024, 1536), (1536, V_TILE)]
            return alternate(out, [functools.partial(feat_piece, l, k0, k1) for l in range(0, t, pn) for k0, k1 in pk])

        @pl.when(s == 0)
        def _():
            interleave([], grads(ga))

        if not whole:
            @pl.when(s == 1)
            def _():
                fetch().wait()

        for parity, (g_old, g_new) in enumerate([(gb, ga), (ga, gb)]):
            mid = (s > 0) & (s < last) & (lax.rem(s, 2) == parity)
            if whole:
                @pl.when(mid)
                def _():
                    interleave(dots(g_old, True), grads(g_new))
            else:
                @pl.when(mid & (pk == nk))
                def _():
                    interleave(dots(g_old, True), grads(g_new))

                @pl.when(mid & (pk < nk))
                def _():
                    interleave(dots(g_old, False), grads(g_new))

        @pl.when(s == last)
        def _():
            interleave(dots(ga if last % 2 == 1 else gb, True), [])
            if not whole:
                dfa_ref[ALL] = df_ref[0]
                dfb_ref[ALL] = df_ref[1]

    def now(s):
        return jnp.minimum(s, last - 1)

    def lag(s):
        return jnp.maximum(s - 1, 0) // nj

    def lag_j(s):
        return lax.rem(jnp.maximum(s - 1, 0), nj)

    by_chunk = pl.BlockSpec((None, 2, WIDTH, half_n), lambda s, c: (lag_j(s) // (TWO * per_half), 0, 0, 0))
    row = pl.BlockSpec((1, n), lambda s, c: (0, at), **once())
    out_blk = pl.BlockSpec((V_TILE, WIDTH), lambda s, c: ORIGIN, **once())
    in_specs = [
        pl.BlockSpec((V_TILE, t), lambda s, c: (tile(c, now(s) // nj), at * nj + lax.rem(now(s), nj))),
        pl.BlockSpec((t, WIDTH), lambda s, c: (at * nj + lag_j(s), 0)),
        pl.BlockSpec((V_TILE, WIDTH), lambda s, c: (c[0] * nv + tile(c, lag(s)), 0)),
        row, row, row,
    ]
    args = [logits, feats, out_tab, lab, le, wt]
    if d_feats is not None:
        in_specs.append(by_chunk if whole else pl.BlockSpec(memory_space=pl.ANY))
        args.append(d_feats)
    if d_out is not None:
        in_specs.append(out_blk)
        args.append(d_out)
    df_shape = (N_CHUNK, 2, WIDTH, half_n) if whole else (WIDTH, half_n)
    df_spec = by_chunk if whole else pl.BlockSpec(df_shape, lambda s, c: ORIGIN, **once())
    df_outs = 1 if whole else 2
    grid_spec = pltpu.PrefetchScalarGridSpec(
        num_scalar_prefetch=1,
        grid=(last + 1,),
        in_specs=in_specs,
        out_specs=[out_blk] + [df_spec] * df_outs + [pl.BlockSpec((PACK, n), lambda s, c: ORIGIN, **once())],
        scratch_shapes=[pltpu.VMEM((V_TILE, t), bf16)] * TWO
        + ([] if whole else [pltpu.VMEM((2, WIDTH, half_n), f32), pltpu.SemaphoreType.DMA(())]),
    )
    return pl.pallas_call(
        body,
        grid_spec=grid_spec,
        out_shape=[jax.ShapeDtypeStruct((V_TILE, WIDTH), f32)] + [jax.ShapeDtypeStruct(df_shape, f32)] * df_outs
        + [jax.ShapeDtypeStruct((PACK, n), f32)],
        compiler_params=params(),
        cost_estimate=cost(2, n_tiles * V_TILE, n, 4 * n_tiles * V_TILE * n),
        name="own",
    )(meta, *args)


def other_kernel(meta, feats, out_tab, lab, le, wt, acc, whole, kept):
    n = feats.shape[0]
    block = out_tab.shape[0]
    nv = block // TWO // V_TILE
    t, lanes, pz, pm, pr = STEP, LANES, 6, 6, 4
    last = n // t

    def tile(m):
        return (nv // TWO) * m[1] + kept

    def body(meta_ref, f_ref, fl_ref, w_ref, lab_ref, le_ref, wt_ref, in_ref, *rest):
        dw_ref, whole_ref, ya, yb, ga, gb = rest[-6:]
        s = pl.program_id(0)

        def start(k):
            return pl.multiple_of(jnp.clip(s - k, 0, last - 1) * t, t)

        row0 = tile(meta_ref) * V_TILE

        def logit_pieces(y):
            def piece(r0, r1):
                y[r0:r1, :] = lax.dot_general(w_ref[r0:r1, :], f_ref[ALL], NT, preferred_element_type=f32)

            return [functools.partial(piece, r0, r1) for r0, r1 in cuts(V_TILE, pz, PACK)]

        def out_pieces(g):
            def piece(r0, r1):
                dw_ref[r0:r1, :] += lax.dot_general(g[r0:r1, :], fl_ref[ALL], NN, preferred_element_type=f32)

            return [functools.partial(piece, r0, r1) for r0, r1 in cuts(V_TILE, pm, PACK)]

        def grads(y, g):
            return [
                functools.partial(grad_piece, y, g, lab_ref, le_ref, wt_ref, None, start(1), row0, lanes, True, l, r0, r1)
                for l in range(0, t, lanes) for r0, r1 in cuts(V_TILE, pr, PACK)
            ]

        @pl.when(s == 0)
        def _():
            dw_ref[ALL] = in_ref[ALL]
            interleave(logit_pieces(ya), [])

        @pl.when(s == 1)
        def _():
            interleave(logit_pieces(yb), grads(ya, ga))

        for parity, (y_new, y_old, g_new, g_old) in enumerate([(ya, yb, gb, ga), (yb, ya, ga, gb)]):
            @pl.when((s > 1) & (s < last) & (lax.rem(s, 2) == parity))
            def _():
                interleave(alternate(logit_pieces(y_new), out_pieces(g_old)), grads(y_old, g_new))

        y_end, g_end, g_pre = (yb, gb, ga) if last % 2 == 0 else (ya, ga, gb)

        @pl.when(s == last)
        def _():
            interleave(out_pieces(g_pre), grads(y_end, g_end))

        @pl.when(s == last + 1)
        def _():
            interleave(out_pieces(g_end), [])
            whole_ref[ALL] = dw_ref[ALL]

    row = pl.BlockSpec((1, n), lambda s, c: ORIGIN, **once())
    out_blk = pl.BlockSpec((V_TILE, WIDTH), lambda s, c: ORIGIN, **once())
    extra = [] if whole is None else [whole]
    grid_spec = pltpu.PrefetchScalarGridSpec(
        num_scalar_prefetch=1,
        grid=(last + 2,),
        in_specs=[
            pl.BlockSpec((t, WIDTH), lambda s, c: (jnp.minimum(s, last - 1), 0)),
            pl.BlockSpec((t, WIDTH), lambda s, c: (jnp.clip(s - 2, 0, last - 1), 0)),
            pl.BlockSpec((V_TILE, WIDTH), lambda s, c: (c[0] * nv + tile(c), 0), **once()),
            row, row, row, out_blk,
        ] + [pl.BlockSpec(memory_space=pl.ANY)] * len(extra),
        out_specs=[out_blk, pl.BlockSpec((V_TILE, WIDTH), lambda s, c: (c[0] * nv + tile(c), 0), **once())],
        scratch_shapes=[pltpu.VMEM((V_TILE, t), f32)] * TWO + [pltpu.VMEM((V_TILE, t), bf16)] * TWO,
    )
    return pl.pallas_call(
        body,
        grid_spec=grid_spec,
        out_shape=[jax.ShapeDtypeStruct((V_TILE, WIDTH), f32), jax.ShapeDtypeStruct((block, WIDTH), f32)],
        input_output_aliases={SUB: 1} if extra else {},
        compiler_params=params(),
        cost_estimate=cost(2, V_TILE, n, 12 * V_TILE * WIDTH),
        name="other",
    )(meta, feats, feats, out_tab, lab, le, wt, acc, *extra)


def row_sums(order, ids, bounds, parts, before, where, tiles, whole, block):
    m, (n, width) = len(parts), parts[0].shape
    unroll, n_put = PACK, len(tiles)
    has_before = before is not None

    def body(order_ref, id_ref, b_ref, where_ref, *rest):
        rest = list(rest)
        ins = [rest.pop(0) for _ in range(m)]
        put = [rest.pop(0) for _ in range(n_put)]
        if n_put:
            rest.pop(0)
        in_ref = rest.pop(0) if has_before else None
        out_ref = rest.pop(0)
        whole_ref = rest.pop(0) if n_put else None
        buf, sem = rest[:2]
        stage, sem_in, sem_out = rest[2:] if n_put else (None, None, None)
        p = pl.program_id(0)

        def fetch(i):
            return pltpu.make_async_copy(ins[i], buf.at[pl.ds(i * n, n)], sem.at[i])

        @pl.when(p == 0)
        def _():
            for i in range(m):
                fetch(i).start()

        def load(i):
            return pltpu.make_async_copy(put[i], stage.at[i % 2], sem_in.at[i % 2])

        def store(i):
            row = pl.multiple_of(where_ref[i], PACK)
            return pltpu.make_async_copy(stage.at[i % 2], whole_ref.at[pl.ds(row, V_TILE)], sem_out.at[i % 2])

        for i in range(n_put + 2 if n_put else 0):
            @pl.when(p == i)
            def _(i=i):
                if i >= 2:
                    store(i - 2).wait()
                if i < n_put:
                    load(i).start()

        out_ref[ALL] = in_ref[ALL] if has_before else jnp.zeros_like(out_ref)

        @pl.when(p == 0)
        def _():
            for i in range(m):
                fetch(i).wait()

        lo, hi = b_ref[p], b_ref[p + 1]

        def one(k, carry):
            prev, acc = carry
            row, d = order_ref[k], id_ref[k]
            at = pl.ds(d - p * V_TILE, 1)
            x = buf[pl.ds(row, 1), :]
            acc = jnp.where(d == prev, acc + x, (in_ref[at, :] + x) if has_before else x)
            out_ref[at, :] = acc
            return d, acc

        def several(i, carry):
            for u in range(unroll):
                carry = one(lo + i * unroll + u, carry)
            return carry

        full = (hi - lo) // unroll
        carry = lax.fori_loop(0, full, several, (jnp.int32(-1), jnp.zeros((1, width), f32)))
        lax.fori_loop(lo + full * unroll, hi, one, carry)

        for i in range(n_put):
            @pl.when(p == i)
            def _(i=i):
                load(i).wait()
                store(i).start()

    rows = pl.BlockSpec((V_TILE, width), lambda p, *_: (p, 0))
    anywhere = pl.BlockSpec(memory_space=pl.ANY)
    extra = list(tiles) + ([whole] if n_put else []) + ([before] if has_before else [])
    aliases = {4 + m + n_put: 1} if n_put else {}
    if has_before:
        aliases[4 + m + len(extra) - 1] = 0
    grid_spec = pltpu.PrefetchScalarGridSpec(
        num_scalar_prefetch=4,
        grid=(block // V_TILE,),
        in_specs=[anywhere] * (m + n_put + (1 if n_put else 0)) + ([rows] if has_before else []),
        out_specs=[rows] + ([anywhere] if n_put else []),
        scratch_shapes=[pltpu.VMEM((m * n, width), f32), pltpu.SemaphoreType.DMA((m,))] + ([
            pltpu.VMEM((2, V_TILE, width), f32), pltpu.SemaphoreType.DMA((2,)), pltpu.SemaphoreType.DMA((2,))] if n_put else []),
    )
    return pl.pallas_call(
        body,
        grid_spec=grid_spec,
        out_shape=[jax.ShapeDtypeStruct((block, width), f32)] + ([jax.ShapeDtypeStruct(whole.shape, f32)] if n_put else []),
        input_output_aliases=aliases,
        compiler_params=params(),
        cost_estimate=pl.CostEstimate(flops=120_000_000, bytes_accessed=4 * (m * n + block) * width, transcendentals=0),
        name="row_sums",
    )(order, ids, bounds, where, *parts, *extra)


def solution(mesh):
    def local_step(hidden, tokens, emb_blk, out_blk, w_proj, gain_h, gain_e, gain_f):
        batch, piece, width = hidden.shape
        block = emb_blk.shape[0]
        rows = block // TWO
        n_own = batch * piece
        n_c = n_own // N_CHUNK
        tp_rank, cp_rank = lax.axis_index("tp"), lax.axis_index("cp")
        core = lax.rem(cp_rank, 2)
        x_rank = cp_rank // TWO
        meta = jnp.stack([core, x_rank])
        seq_len = piece * 4
        row_start = tp_rank * block + core * rows

        def core_swap(v):
            return lax.ppermute(v, "cp", CORE_SWAP)

        def x_swap(v):
            return lax.ppermute(v, "cp", X_SWAP)

        def y_swap(v):
            return lax.ppermute(v, "tp", Y_SWAP)

        def weights_of(first):
            ranks = cp_rank ^ (first + jnp.arange(2))
            pos = ranks[:, None] * piece + jnp.arange(piece)[None, :]
            w = MTP_WEIGHT * (pos < seq_len - 2).astype(f32)
            return jnp.broadcast_to(w[None, :, None, :], (N_CHUNK, 2, batch // N_CHUNK, piece)).reshape(1, -1)

        head = lax.ppermute(tokens[:, :2], "cp", [(k + 1, k) for k in range(3)])
        ahead = jnp.concatenate([tokens, head], axis=1)
        ids_own = jnp.stack([ahead[:, 1:piece + 1], ahead[:, 2:]]).reshape(2, N_CHUNK, n_c)
        ids_mate = core_swap(ids_own)
        ids_far = x_swap(ids_own)
        ids_diag = core_swap(ids_far)
        next_ids = [v[0] for v in (ids_own, ids_mate, ids_far, ids_diag)]
        labels = [v[1] - row_start for v in (ids_own, ids_mate, ids_far, ids_diag)]
        wt_own, wt_far = weights_of(0), weights_of(2)

        local_next = next_ids[0] - tp_rank * block
        in_block = (local_next >= 0) & (local_next < block)
        take = jnp.clip(local_next, 0, block - 1)
        hid = hidden.reshape(N_CHUNK, n_c, width)

        emb_own, emb_recv = [], []
        for c in range(N_CHUNK):
            e = jnp.where(in_block[c][:, None], jnp.take(emb_blk, take[c], axis=0).astype(f32), 0.0)
            emb_own.append(e)
            emb_recv.append(y_swap(e))

        starts = jnp.arange(block // V_TILE + 1) * V_TILE

        def sorted_ids(chunks):
            ids = jnp.concatenate([next_ids[k][c] for k in (0, 2, 1, 3) for c in chunks]) - tp_rank * block
            seg = jnp.where((ids >= 0) & (ids < block), ids, block)
            seg_sorted, order = lax.sort((seg, jnp.arange(seg.shape[0], dtype=jnp.int32)), num_keys=1)
            bounds = jnp.sum(seg[None, :] < starts[:, None], axis=1).astype(jnp.int32)
            return order, seg_sorted, bounds

        first_ids, last_ids = sorted_ids(range(N_CHUNK - 1)), sorted_ids([N_CHUNK - 1])

        gains = jnp.stack([gain_h, gain_e, gain_f])
        far_parts, f_own, logits, stats = [], None, None, []
        for c in range(N_CHUNK):
            normed = front_kernel(hid[c], emb_own[c], emb_recv[c], w_proj, gains)
            mate = core_swap(normed)
            f_own = round_rows([normed, mate], TWO * n_own, c, f_own)
            far = x_swap(normed)
            far_parts += [far, core_swap(far)]
            logits, st = logits_kernel(meta, out_blk, f_own, rows, c, logits)
            stats.append(st)

        log_sums = ()
        for c in range(N_CHUNK):
            recv = core_swap(stats[c])
            both = merge_halves(stats[c], recv)
            recv = y_swap(both)
            log_sums = finish_stats(both, recv, wt_own, c, log_sums)
        lse_own, le_own = log_sums
        le_far = x_swap(le_own)

        lab_own = jnp.stack(labels[:2], axis=1).reshape(1, -1)
        lab_far = jnp.stack(labels[2:], axis=1).reshape(1, -1)
        own_args = (meta, logits, f_own, out_blk, lab_own, le_own, wt_own)
        f_far = round_rows(far_parts)
        far_args = (meta, f_far, out_blk, lab_far, le_far, wt_far)

        n_kept = rows // V_TILE // TWO
        whole, df_sum, hits, mates = None, None, 0.0, []

        def finish(kept, d_out, whole):
            mine, whole = other_kernel(*far_args, d_out, whole, kept)
            mate = core_swap(mine)
            far = x_swap(mine)
            mates.append((mate, far, core_swap(far)))
            return whole

        for kept in range(n_kept - 1):
            d_out, df_sum, hit = own_kernel(*own_args, kept, None, df_sum, None)
            hits += jnp.sum(wt_own * hit)
            whole = finish(kept, d_out, whole)

        df_terms, d_out = [], None
        for c in range(N_CHUNK):
            d_out, df_own, df_mate, hit = own_kernel(*own_args, n_kept - 1, c, df_sum, d_out)
            hits += jnp.sum(wt_own.reshape(N_CHUNK, 1, -1)[c] * hit)
            recv = core_swap(df_mate)
            mine = df_own + recv
            recv = y_swap(mine)
            df_terms.append((mine, recv))
        whole = finish(n_kept - 1, d_out, whole)

        totals, de_own, de_far, de_mate, de_diag = (), [], [], [], []
        for c in range(N_CHUNK):
            d_hid, de, *sums = back_kernel(hid[c], emb_own[c], emb_recv[c], w_proj, gains, *df_terms[c], c, totals)
            totals = (*sums, d_hid)
            de_own.append(de)
            de_far.append(x_swap(de))
            de_mate.append(core_swap(de))
            de_diag.append(core_swap(de_far[c]))

        mine = (wt_own * lse_own).reshape(N_CHUNK, 2, -1)[:, 0]
        loss_part = 0.5 * jnp.sum(mine) - hits
        d_proj = totals[0]
        small = jnp.concatenate([jnp.sum(totals[1].reshape(3, SUB, width), axis=1), jnp.full((5, width), loss_part)], axis=0)
        half_rows = width // TWO
        mine = lax.dynamic_slice(d_proj, (core * half_rows, 0), (half_rows, TWO * width))
        theirs = lax.dynamic_slice(d_proj, ((1 - core) * half_rows, 0), (half_rows, TWO * width))
        mine, small = mine + core_swap(theirs), small + core_swap(small)
        mine, small = mine + x_swap(mine), small + x_swap(small)
        theirs = core_swap(mine)
        d_proj = lax.dynamic_update_slice(d_proj, mine, (core * half_rows, 0))
        d_proj = lax.dynamic_update_slice(d_proj, theirs, ((1 - core) * half_rows, 0))
        loss_sum = small[3:4, 0] + y_swap(small[3:, :128])[0:1, 0]

        places = []
        for kept in range(n_kept):
            for which, v in enumerate(mates[kept]):
                core_of = core if which == 1 else 1 - core
                x_of = x_rank if which == 0 else 1 - x_rank
                places.append((core_of * rows + (n_kept * x_of + kept) * V_TILE, v))
        early, late = places[:-2], places[-2:]
        kinds = (de_own, de_far, de_mate, de_diag)
        where = jnp.stack([p[0] for p in early])
        d_emb, whole = row_sums(
            *first_ids, [v for kind in kinds for v in kind[:-1]], None, where, [p[1] for p in early], whole, block)
        d_emb, = row_sums(*last_ids, [kind[-1] for kind in kinds], d_emb, where, [], None, block)
        for start, v in late:
            whole = lax.dynamic_update_slice(whole, v, (start, 0))

        loss = LN2 * loss_sum / (batch * (seq_len - 2))
        d_hidden = d_hid.reshape(batch, piece, width)
        return loss, d_hidden, d_proj, d_emb, whole, small[0], small[1], small[2]

    part_seq = P("dp", "cp", None)
    in_specs = (part_seq, P("dp", "cp"), P("tp", None), P("tp", None), P(None, None), P(None), P(None), P(None))
    out_specs = (P("dp"), part_seq, P("dp", None), P(("dp", "tp"), None), P(("dp", "tp"), None), P("dp"), P("dp"), P("dp"))
    return jax.shard_map(local_step, mesh=mesh, in_specs=in_specs, out_specs=out_specs, check_vma=False)
```
